32 devices in a mesh: row: 8 (over z, y), col: 4 (over x, core).
Axes of the slice: x: 2, y: 2, z: 4, core: 2. Of those that a mesh axis runs over, the one named last changes fastest.
Arguments:
- grads: float32 [64, 20, 3, 4096], P(None, None, None, ('row', 'col')), may hold values from -6 to 6
- weights: float32 [64, 4096], P(None, ('row', 'col')), may hold values from 0.005 to 0.05
- counts: int32 [4096], P(('row', 'col')), may hold values from 1 to 8
- lame_first: float32 [4096], P(('row', 'col')), may hold values from 0.5 to 2
- shear: float32 [4096], P(('row', 'col')), may hold values from 0.5 to 2
- dest_owner: int32 [4096, 1], P(('row', 'col')), may hold values from 0 to 31; in each aligned block of 128 rows (0 to 127, 128 to 255, ...) at most 8 rows name the same one
- dest_slot: int32 [4096], P(('row', 'col')), may hold values from 0 to 127
Outputs:
- assembled: float32 [60, 60, 4096], P(None, None, ('row', 'col'))
The draws below stay inside these ranges and needn't reach their ends.
Inputs may be any that keep to these rules, and one draw needn't show every extreme that they name: `dest_owner`: among the elements of one device, at most 8 have the same owner; in some device exactly 8 do.
All inputs are finite; a program needn't handle non-finite values.
Results may differ from the reference program's by a relative error of at most 0.0001.
Values sent between devices are 32-bit elements; how exact they have to be, the bound alone decides.
A program may use at most 64 MiB of HBM per device.

```python
import math
import jax
import jax.numpy as jnp
import numpy as np
from jax import lax

NF = 20
NDOF = 60
GP = 8
SUBMAX = 8
Q = 64
E_DEV = 128
SLOTS_DEV = 128
ELEMS = 4096
SLOTS = 4096
CAP = 8
N_ROW = 8
N_COL = 4
DEVICES = 32


def plant(entries, rng, low, high):
    longest = entries.shape.index(max(entries.shape))
    spots = []
    for shift in (0, 1):
        where = [jax.random.randint(jax.random.fold_in(rng, axis), (), 0, length) for axis, length in enumerate(entries.shape)]
        where[longest] = (where[longest] + shift) % entries.shape[longest]
        spots.append(tuple(where))
    return entries.at[spots[0]].set(low).at[spots[1]].set(high)


def steps_of(stream_key, dims, split, smallest, high):
    def one(position, shards_of):
        draws = jax.random.uniform(jax.random.fold_in(jax.random.fold_in(stream_key, 6), position), (shards_of,), jnp.float32, smallest / len(split), high / len(split))
        return jnp.repeat(jnp.exp(draws), dims[position] // shards_of).reshape((-1,) + (1,) * (len(dims) - position - 1))

    gain = one(*split[0])
    for cut in split[1:]:
        gain = gain * one(*cut)
    return gain


def assign_block(rng, own, number, rows, number_of, top, limit, skew):
    order = jax.random.permutation(rng, number_of)
    crowded, usual = load_shares(number_of, rows * top, limit, skew, True), load_shares(number_of, rows * top, limit, skew, False)
    places = jnp.arange(number_of)

    def named(lengths, turn):
        used = int((lengths > 0).sum())
        fixed = max(1, used // 4)
        moved = fixed + (places - fixed + turn * (used - fixed)) % max(1, number_of - fixed)
        return jnp.zeros((number_of,), jnp.int32).at[order[jnp.where(places < fixed, places, moved)]].set(jnp.asarray(lengths, jnp.int32))

    lengths = jnp.where(number % 4 == 0, named(crowded, number // 4), named(usual, number - number // 4 - 1))
    mixed = jax.random.permutation(jax.random.fold_in(own, 3), number_of)
    giver, sink = mixed[0:number_of // 2 * 2:2], mixed[1:number_of // 2 * 2:2]
    margin = jnp.minimum(lengths[giver] - 1, limit - lengths[sink]) // 2
    margin = jnp.where((giver == order[0]) | (sink == order[0]) | (lengths[sink] == 0), 0, jnp.maximum(margin, 0))
    moved = jax.random.randint(jax.random.fold_in(own, 4), (number_of // 2,), 0, 1 << 20) % (margin + 1)
    lengths = lengths.at[giver].add(-moved).at[sink].add(moved)
    members = jnp.searchsorted(jnp.cumsum(lengths), jnp.arange(rows * top), side="right").astype(jnp.int32)
    listing = members.reshape(top, rows).T
    listing = listing[jax.random.permutation(jax.random.fold_in(own, 1), rows)]
    turn = jax.random.randint(jax.random.fold_in(own, 2), (rows, 1), 0, top)
    return jnp.take_along_axis(listing, (jnp.arange(top)[None, :] + turn) % top, axis=1)


def load_shares(number_of, total, reach, lean, full):
    weights = [(1 << 20) // math.isqrt(rank ** lean) + 1 for rank in range(1, number_of + 1)]
    largest = reach if full else min(reach, max(-(-total // number_of), total * weights[0] // sum(weights)))
    least = 1 if total - largest >= number_of - 1 else 0
    given, surplus = [largest] + [least] * (number_of - 1), total - largest - least * (number_of - 1)
    while surplus > 0:
        free = [i for i in range(1, number_of) if given[i] < largest] or [i for i in range(1, number_of) if given[i] < reach]
        pool, budget = sum([weights[i] for i in free]), surplus
        for i in free:
            addition = min(reach - given[i], max(1, budget * weights[i] // pool), surplus)
            given[i] = given[i] + addition
            surplus = surplus - addition
    return np.array(given)


def normal_values(rng, shape, scale, limit, shards=(), held_as=jnp.bfloat16):
    values = scale * jax.random.normal(rng, shape, jnp.float32)
    if shards:
        values = values * steps_of(rng, shape, shards, -0.22, 0.18)
    return jnp.clip(values, -limit, limit).astype(held_as)


def setup_inputs(seed: int = 0) -> dict:
    key_of = jax.random.split(jax.random.key(seed), 8)
    grads = normal_values(key_of[0], (Q, NF, 3, ELEMS), 1.0, 6.0, ((3, 32),), jnp.float32)
    weights = jnp.clip(jnp.exp(math.log(0.05) - 2.3025851 * jax.random.uniform(key_of[1], (Q, ELEMS), jnp.float32) ** steps_of(key_of[1], (Q, ELEMS), ((1, 32),), -0.2, 0.2)), 0.005, 0.05)
    counts = plant(jax.random.randint(key_of[2], (ELEMS,), 1, SUBMAX + 1), jax.random.fold_in(key_of[2], 1), 1, SUBMAX).astype(jnp.int32)
    lame_first = jnp.clip(jnp.exp(math.log(2.0) - 1.3862944 * jax.random.uniform(key_of[3], (ELEMS,), jnp.float32) ** steps_of(key_of[3], (ELEMS,), ((0, 32),), -0.2, 0.2)), 0.5, 2.0)
    shear = jnp.clip(jnp.exp(math.log(2.0) - 1.3862944 * jax.random.uniform(key_of[4], (ELEMS,), jnp.float32) ** steps_of(key_of[4], (ELEMS,), ((0, 32),), -0.2, 0.2)), 0.5, 2.0)
    dest_owner_keys = jax.random.split(jax.random.fold_in(key_of[5], 1), ELEMS // E_DEV)
    dest_owner_turns = jax.random.permutation(jax.random.fold_in(key_of[5], 3), ELEMS // E_DEV)
    dest_owner = jax.vmap(lambda own, number: assign_block(jax.random.fold_in(key_of[5], 2), own, number, E_DEV, DEVICES, 1, CAP, 2))(dest_owner_keys, dest_owner_turns).reshape((ELEMS, 1))
    dest_slot = plant(jax.random.randint(key_of[6], (ELEMS,), 0, SLOTS_DEV), jax.random.fold_in(key_of[6], 1), 0, SLOTS_DEV - 1).astype(jnp.int32)
    return dict(grads=grads, weights=weights, counts=counts, lame_first=lame_first, shear=shear, dest_owner=dest_owner, dest_slot=dest_slot)


def stiffness(gflat, weff, lame_first, shear):
    count = gflat.shape[2]
    moment = jnp.einsum("qme,qne->mne", gflat * weff[:, None, :], gflat, precision=lax.Precision.HIGHEST)
    blocks = moment.reshape(NF, 3, NF, 3, count)
    across = jnp.einsum("akbke->abe", blocks)
    eye = jnp.eye(3, dtype=jnp.float32)
    result = lame_first * blocks + shear * (eye[None, :, None, :, None] * across[:, None, :, None, :] + jnp.transpose(blocks, (0, 3, 2, 1, 4)))
    return result.reshape(NDOF * NDOF, count)


def reference(grads, weights, counts, lame_first, shear, dest_owner, dest_slot):
    points = lax.broadcasted_iota(jnp.int32, weights.shape, 0)
    weff = jnp.where(points < counts[None, :] * GP, weights, jnp.float32(0.0))
    squares = jnp.sum(grads * grads, axis=(1, 2))
    total = jnp.sum((lame_first + 4.0 * shear) * jnp.sum(weff * squares, axis=0))
    scale = total / (NDOF * ELEMS)
    target = (dest_owner[:, 0] * SLOTS_DEV + dest_slot).astype(jnp.int32)
    gflat = grads.reshape(Q, NDOF, ELEMS)

    def add_block(index, accum):
        start = (index * E_DEV).astype(jnp.int32)
        gpart = lax.dynamic_slice_in_dim(gflat, start, E_DEV, 2)
        wpart = lax.dynamic_slice_in_dim(weff, start, E_DEV, 1)
        lpart = lax.dynamic_slice_in_dim(lame_first, start, E_DEV, 0)
        spart = lax.dynamic_slice_in_dim(shear, start, E_DEV, 0)
        tpart = lax.dynamic_slice_in_dim(target, start, E_DEV, 0)
        return accum.at[:, tpart].add(stiffness(gpart, wpart, lpart, spart))

    accum = lax.fori_loop(0, N_ROW * N_COL, add_block, jnp.zeros((NDOF * NDOF, SLOTS), jnp.float32))
    return (accum / scale).reshape(NDOF, NDOF, SLOTS)
```

```python
import functools

import jax
import jax.numpy as jnp
from jax import lax
from jax.experimental import pallas as pl
from jax.experimental.pallas import tpu as pltpu
from jax.sharding import PartitionSpec as P

GP = 8
LANES = 128
CHUNKS = 3
F32 = jnp.float32
BF16 = jnp.bfloat16
NT = (((1,), (1,)), ((), ()))


def split2(x):
    high = x.astype(BF16)
    return high, (x - high.astype(F32)).astype(BF16)


def row_base(d, nodes, pair):
    half = nodes // 2
    if d < half:
        return d * 9 * nodes + pair * nodes, nodes
    return half * 9 * nodes + pair * half, half


def send_kernel(sizes, grads, weights, counts, lame, shear, owner, slot, recv,
                gbuf, wbuf, kbuf, send, ssem, rsem, lsem):
    nodes, nq, nrow, ncol, cap, packed, total_rows = sizes
    ndev = nrow * ncol
    width = ndev * cap
    half = nodes // 2
    clen = total_rows // CHUNKS
    me = lax.axis_index("row") * ncol + lax.axis_index("col")

    def device(k):
        t = lax.rem(me + k, ndev)
        return t, (t // ncol, lax.rem(t, ncol))

    barrier = pltpu.get_barrier_semaphore()

    @pl.loop(1, ndev)
    def _(k):
        pl.semaphore_signal(barrier, inc=1, device_id=device(k)[1],
                            device_id_type=pl.DeviceIdType.MESH)

    span = 2 * nodes
    pad = 24

    def prepare(q, carry):
        weight = weights[pl.ds(q, 1), :]
        weight = jnp.where(q < counts[...] * GP, weight, 0.0)
        for i in range(3):
            values = grads[pl.ds(i * nq + q, nodes, stride=3 * nq), :]
            gbuf[q, pl.ds(i * span, nodes), :] = values
            gbuf[q, pl.ds(i * span + nodes, nodes), :] = values
            wbuf[q, pl.ds(i * pad, nodes), :] = values * weight
        return carry

    lax.fori_loop(0, nq, prepare, 0, unroll=4)

    who = owner[...].astype(F32)
    across = jnp.broadcast_to(who, (LANES, LANES))
    down = across.T
    first = lax.broadcasted_iota(jnp.int32, (LANES, LANES), 0)
    second = lax.broadcasted_iota(jnp.int32, (LANES, LANES), 1)
    same = jnp.where((across == down) & (first < second), 1.0, 0.0)
    rank = jnp.sum(same, axis=0, keepdims=True)
    position = (who * cap + rank).astype(jnp.int32)
    where = lax.broadcasted_iota(jnp.int32, (width, LANES), 0)
    onehot = jnp.where(where == position, 1.0, 0.0).astype(BF16)
    onehot2 = jnp.concatenate([onehot, onehot], axis=1)

    lam, mu = lame[...], shear[...]
    trace_row = jnp.zeros((1, LANES), F32)
    tail = total_rows - packed
    extra = lax.broadcasted_iota(jnp.int32, (tail, LANES), 0)
    kbuf[pl.ds(packed, tail), :] = jnp.where(extra == 0, slot[...].astype(F32) + 1.0, 0.0)

    chunk = 0
    for d in range(half + 1):
        tiles = 3 if d < half else 2

        def step(q, acc, d=d, tiles=tiles):
            acc = list(acc)
            for t in range(tiles):
                left = [wbuf[q, pl.ds(i * pad + 8 * t, 8), :] for i in range(3)]
                right = [gbuf[q, pl.ds(j * span + d + 8 * t, 8), :] for j in range(3)]
                for i in range(3):
                    for j in range(3):
                        n = t * 9 + 3 * i + j
                        acc[n] = acc[n] + left[i] * right[j]
            return tuple(acc)

        zero = jnp.zeros((8, LANES), F32)
        acc = lax.fori_loop(0, nq, step, (zero,) * (9 * tiles), unroll=2)
        for t in range(tiles):
            m = acc[9 * t: 9 * t + 9]
            diag = m[0] + m[4] + m[8]
            _, length = row_base(d, nodes, 0)
            rows = min(8, length - 8 * t)
            if d == 0:
                trace_row = trace_row + jnp.sum(diag[:rows], axis=0, keepdims=True)
            for i in range(3):
                for j in range(3):
                    value = lam * m[3 * i + j] + mu * m[3 * j + i]
                    if i == j:
                        value = value + mu * diag
                    base, _ = row_base(d, nodes, 3 * i + j)
                    kbuf[pl.ds(base + 8 * t, rows), :] = value[:rows]
        if d == 0:
            local = jnp.sum((lam + 4.0 * mu) * trace_row, axis=(0, 1), keepdims=True)
        done = packed if d == half else 9 * nodes * (d + 1)
        while chunk < CHUNKS and (done >= (chunk + 1) * clen or d == half):
            high, low = split2(kbuf[pl.ds(chunk * clen, clen), :])
            both = jnp.concatenate([high, low], axis=1)
            out = lax.dot_general(onehot2, both, NT, preferred_element_type=F32)
            if chunk == CHUNKS - 1:
                column = lax.broadcasted_iota(jnp.int32, (width, clen), 1)
                out = jnp.where(column == packed + 1 - chunk * clen, local, out)
            send[chunk] = out
            if chunk == 0:
                pl.semaphore_wait(barrier, ndev - 1)

            @pl.loop(1, ndev)
            def _(k, chunk=chunk):
                t, where_to = device(k)
                pltpu.make_async_remote_copy(
                    src_ref=send.at[chunk, pl.ds(pl.multiple_of(t * cap, 8), cap)],
                    dst_ref=recv.at[chunk, pl.ds(pl.multiple_of(me * cap, 8), cap)],
                    send_sem=ssem.at[chunk], recv_sem=rsem.at[chunk],
                    device_id=where_to, device_id_type=pl.DeviceIdType.MESH).start()

            mine = pl.ds(pl.multiple_of(me * cap, 8), cap)
            pltpu.make_async_copy(send.at[chunk, mine], recv.at[chunk, mine],
                                  lsem.at[chunk]).start()
            chunk += 1

    for c in range(CHUNKS):
        mine = pl.ds(pl.multiple_of(me * cap, 8), cap)
        pltpu.make_async_copy(send.at[c, mine], recv.at[c, mine], lsem.at[c]).wait()
        most = pl.ds(0, (ndev - 1) * cap)
        pltpu.make_async_copy(send.at[c, most], send.at[c, most], ssem.at[c]).wait()
        pltpu.make_async_copy(recv.at[c, most], recv.at[c, most], rsem.at[c]).wait()


def place_kernel(sizes, recv, out, tbuf):
    nodes, ndof, cap, packed, total_rows, count_all = sizes
    clen = total_rows // CHUNKS
    half = nodes // 2
    pitch = ndof + (-ndof) % 8
    last = recv[CHUNKS - 1]
    start = (packed - (CHUNKS - 1) * clen) // LANES * LANES
    inner = packed - (CHUNKS - 1) * clen - start
    info = last[:, start:start + LANES]
    width = info.shape[0]
    slots = info[:, inner:inner + 1]
    total = jnp.sum(info[:, inner + 1:inner + 2], axis=0, keepdims=True) / cap
    inverse = (ndof * count_all) / total
    lane = lax.broadcasted_iota(jnp.int32, (width, LANES), 1)
    placing = jnp.where(slots.astype(jnp.int32) == lane + 1, 1.0, 0.0)
    placing = placing.T.astype(BF16)
    for c in range(CHUNKS):
        high, low = split2(recv[c])
        summed = jnp.dot(placing, high, preferred_element_type=F32)
        summed = summed + jnp.dot(placing, low, preferred_element_type=F32)
        tbuf[pl.ds(c * clen, clen), :] = (summed * inverse).T
    for d in range(half + 1):
        for i in range(3):
            for j in range(3):
                base, length = row_base(d, nodes, 3 * i + j)
                pieces = [(0, min(length, nodes - d), d)]
                if length > nodes - d:
                    pieces.append((nodes - d, length, d - nodes))
                for begin, end, shift in pieces:
                    for a in range(begin, end, 8):
                        n = min(8, end - a)
                        value = tbuf[pl.ds(base + a, n), :]
                        m0, n0 = 3 * a + i, 3 * (a + shift) + j
                        stride = 3 * pitch + 3
                        if n == 1:
                            out[pl.ds(m0 * pitch + n0, 1), :] = value
                            out[pl.ds(n0 * pitch + m0, 1), :] = value
                        else:
                            out[pl.ds(m0 * pitch + n0, n, stride=stride), :] = value
                            if d > 0:
                                out[pl.ds(n0 * pitch + m0, n, stride=stride), :] = value


def shards(nrow, ncol, grads, weights, counts, lame_first, shear, dest_owner, dest_slot):
    nq, nodes, _, count = grads.shape
    ndev = nrow * ncol
    ndof = 3 * nodes
    cap = max(2, 2 * count // ndev)
    cap = cap + (-cap) % 8
    width = ndev * cap
    half = nodes // 2
    packed = 9 * nodes * half + 9 * half
    unit = LANES * CHUNKS
    total_rows = packed + 2
    total_rows = total_rows + (-total_rows) % unit
    clen = total_rows // CHUNKS
    pitch = ndof + (-ndof) % 8
    gview = jnp.transpose(grads, (1, 2, 0, 3)).reshape(ndof * nq, count)
    row = lambda x: x.reshape(1, count)
    vmem = pl.BlockSpec(memory_space=pltpu.VMEM)
    recv = pl.pallas_call(
        functools.partial(send_kernel, (nodes, nq, nrow, ncol, cap, packed, total_rows)),
        out_shape=jax.ShapeDtypeStruct((CHUNKS, width, clen), F32),
        in_specs=[vmem] * 7,
        out_specs=vmem,
        scratch_shapes=[
            pltpu.VMEM((nq, 6 * nodes, LANES), F32),
            pltpu.VMEM((nq, 72, LANES), F32),
            pltpu.VMEM((total_rows, LANES), F32),
            pltpu.VMEM((CHUNKS, width, clen), F32),
            pltpu.SemaphoreType.DMA((CHUNKS,)),
            pltpu.SemaphoreType.DMA((CHUNKS,)),
            pltpu.SemaphoreType.DMA((CHUNKS,)),
        ],
        compiler_params=pltpu.CompilerParams(
            collective_id=0, has_side_effects=True, vmem_limit_bytes=56 << 20),
        name="moments_send",
    )(gview, weights, row(counts), row(lame_first), row(shear), row(dest_owner), row(dest_slot))
    out = pl.pallas_call(
        functools.partial(place_kernel, (nodes, ndof, cap, packed, total_rows, count * ndev)),
        out_shape=jax.ShapeDtypeStruct((ndof * pitch, LANES), F32),
        in_specs=[vmem],
        out_specs=vmem,
        scratch_shapes=[pltpu.VMEM((total_rows, LANES), F32)],
        compiler_params=pltpu.CompilerParams(vmem_limit_bytes=56 << 20),
        name="place",
    )(recv)
    return out.reshape(ndof, pitch, LANES)[:, :ndof, :]


def solution(mesh):
    both = ("row", "col")
    in_specs = (P(None, None, None, both), P(None, both), P(both), P(both), P(both),
                P(both, None), P(both))
    body = functools.partial(shards, mesh.shape["row"], mesh.shape["col"])
    return jax.shard_map(body, mesh=mesh, in_specs=in_specs, out_specs=P(None, None, both),
                         check_vma=False)
```

```python
import functools

import jax
import jax.numpy as jnp
from jax import lax
from jax.experimental import pallas as pl
from jax.experimental.pallas import tpu as pltpu
from jax.sharding import PartitionSpec as P

GP = 8
LANES = 128
HEAD = 8
TILES = (1, 2, 4, 6)
F32 = jnp.float32
BF16 = jnp.bfloat16
NT = (((1,), (1,)), ((), ()))


def split2(x):
    high = x.astype(BF16)
    return high, (x - high.astype(F32)).astype(BF16)


def row_base(d, nodes, i, j):
    half = nodes // 2
    if d == 0:
        i, j = min(i, j), max(i, j)
        return HEAD + (3 * i - i * (i + 1) // 2 + j) * nodes, nodes
    start = HEAD + 6 * nodes + (d - 1) * 9 * nodes
    if d < half:
        return start + (3 * i + j) * nodes, nodes
    return start + (3 * i + j) * half, half


def chunk_bounds(total_rows):
    cuts = [0]
    for tiles in TILES:
        if cuts[-1] + tiles * LANES < total_rows:
            cuts.append(cuts[-1] + tiles * LANES)
    return tuple(zip(cuts, cuts[1:] + [total_rows]))


def send_kernel(sizes, grads, weights, counts, lame, shear, owner, slot, sums,
                gbuf, wbuf, kbuf, send, recv, ssem, rsem, lsem):
    nodes, nq, nrow, ncol, cap, packed, total_rows, count_all = sizes
    ndev = nrow * ncol
    width = ndev * cap
    half = nodes // 2
    chunks = chunk_bounds(total_rows)
    me = lax.axis_index("row") * ncol + lax.axis_index("col")
    mine = pl.ds(pl.multiple_of(me * cap, 8), cap)
    most = pl.ds(0, (ndev - 1) * cap)

    def device(k):
        t = lax.rem(me + k, ndev)
        return t, (t // ncol, lax.rem(t, ncol))

    barrier = pltpu.get_barrier_semaphore()

    @pl.loop(1, ndev)
    def _(k):
        pl.semaphore_signal(barrier, inc=1, device_id=device(k)[1],
                            device_id_type=pl.DeviceIdType.MESH)

    span = 2 * nodes
    pad = 24

    def prepare(q, carry):
        weight = weights[pl.ds(q, 1), :]
        weight = jnp.where(q < counts[...] * GP, weight, 0.0)
        for i in range(3):
            values = grads[pl.ds(i * nq + q, nodes, stride=3 * nq), :]
            gbuf[q, pl.ds(i * span, nodes), :] = values
            gbuf[q, pl.ds(i * span + nodes, nodes), :] = values
            wbuf[q, pl.ds(i * pad, nodes), :] = values * weight
        return carry

    lax.fori_loop(0, nq, prepare, 0, unroll=4)

    who = owner[...].astype(F32)
    across = jnp.broadcast_to(who, (LANES, LANES))
    down = across.T
    first = lax.broadcasted_iota(jnp.int32, (LANES, LANES), 0)
    second = lax.broadcasted_iota(jnp.int32, (LANES, LANES), 1)
    same = jnp.where((across == down) & (first < second), 1.0, 0.0)
    rank = jnp.sum(same, axis=0, keepdims=True)
    position = (who * cap + rank).astype(jnp.int32)
    where = lax.broadcasted_iota(jnp.int32, (width, LANES), 0)
    onehot = jnp.where(where == position, 1.0, 0.0).astype(BF16)
    onehot2 = jnp.concatenate([onehot, onehot], axis=1)

    lam, mu = lame[...], shear[...]
    trace_row = jnp.zeros((1, LANES), F32)
    extra = lax.broadcasted_iota(jnp.int32, (HEAD, LANES), 0)
    kbuf[pl.ds(0, HEAD), :] = jnp.where(extra == 0, slot[...].astype(F32) + 1.0, 0.0)
    kbuf[pl.ds(packed, total_rows - packed), :] = jnp.zeros((total_rows - packed, LANES), F32)

    chunk = 0
    for d in range(half + 1):
        tiles = 3 if d < half else 2

        def step(q, acc, d=d, tiles=tiles):
            acc = list(acc)
            for t in range(tiles):
                left = [wbuf[q, pl.ds(i * pad + 8 * t, 8), :] for i in range(3)]
                right = [gbuf[q, pl.ds(j * span + d + 8 * t, 8), :] for j in range(3)]
                for i in range(3):
                    for j in range(3):
                        n = t * 9 + 3 * i + j
                        acc[n] = acc[n] + left[i] * right[j]
            return tuple(acc)

        zero = jnp.zeros((8, LANES), F32)
        acc = lax.fori_loop(0, nq, step, (zero,) * (9 * tiles), unroll=2)
        for t in range(tiles):
            m = acc[9 * t: 9 * t + 9]
            diag = m[0] + m[4] + m[8]
            _, length = row_base(d, nodes, 0, 0)
            rows = min(8, length - 8 * t)
            if d == 0:
                trace_row = trace_row + jnp.sum(diag[:rows], axis=0, keepdims=True)
            for i in range(3):
                for j in range(i if d == 0 else 0, 3):
                    value = lam * m[3 * i + j] + mu * m[3 * j + i]
                    if i == j:
                        value = value + mu * diag
                    base, _ = row_base(d, nodes, i, j)
                    kbuf[pl.ds(base + 8 * t, rows), :] = value[:rows]
        if d == 0:
            local = jnp.sum((lam + 4.0 * mu) * trace_row, axis=(0, 1), keepdims=True)
        done = total_rows if d == half else HEAD + 6 * nodes + 9 * nodes * d
        while chunk < len(chunks) and chunks[chunk][1] <= done:
            low_row, high_row = chunks[chunk]
            columns = pl.ds(low_row, high_row - low_row)
            high, low = split2(kbuf[columns, :])
            both = jnp.concatenate([high, low], axis=1)
            out = lax.dot_general(onehot2, both, NT, preferred_element_type=F32)
            if chunk == 0:
                column = lax.broadcasted_iota(jnp.int32, out.shape, 1)
                out = jnp.where(column == 1, local, out)
            send[:, columns] = out
            if chunk == 0:
                pl.semaphore_wait(barrier, ndev - 1)

            @pl.loop(1, ndev)
            def _(k, chunk=chunk, columns=columns):
                t, where_to = device(k)
                pltpu.make_async_remote_copy(
                    src_ref=send.at[pl.ds(pl.multiple_of(t * cap, 8), cap), columns],
                    dst_ref=recv.at[mine, columns],
                    send_sem=ssem.at[chunk], recv_sem=rsem.at[chunk],
                    device_id=where_to, device_id_type=pl.DeviceIdType.MESH).start()

            pltpu.make_async_copy(send.at[mine, columns], recv.at[mine, columns],
                                  lsem.at[chunk]).start()
            chunk += 1

    for c, (low_row, high_row) in enumerate(chunks):
        columns = pl.ds(low_row, high_row - low_row)
        pltpu.make_async_copy(send.at[mine, columns], recv.at[mine, columns], lsem.at[c]).wait()
        pltpu.make_async_copy(recv.at[most, columns], recv.at[most, columns], rsem.at[c]).wait()
        if c == 0:
            info = recv[:, 0:LANES]
            total = jnp.sum(info[:, 1:2], axis=0, keepdims=True) / cap
            inverse = (3 * nodes * count_all) / total
            lane = lax.broadcasted_iota(jnp.int32, (width, LANES), 1)
            placing = jnp.where(info[:, 0:1].astype(jnp.int32) == lane + 1, 1.0, 0.0)
            placing = placing.T.astype(BF16)
        high, low = split2(recv[:, columns])
        summed = jnp.dot(placing, high, preferred_element_type=F32)
        summed = summed + jnp.dot(placing, low, preferred_element_type=F32)
        sums[columns, :] = (summed * inverse).T
    for c, (low_row, high_row) in enumerate(chunks):
        columns = pl.ds(low_row, high_row - low_row)
        pltpu.make_async_copy(send.at[most, columns], send.at[most, columns], ssem.at[c]).wait()


def mirror_kernel(nodes, sums, out):
    half = nodes // 2
    ndof = 3 * nodes
    pitch = ndof + (-ndof) % 8
    for d in range(half + 1):
        for i in range(3):
            for j in range(3):
                base, length = row_base(d, nodes, i, j)
                pieces = [(0, min(length, nodes - d), d)]
                if length > nodes - d:
                    pieces.append((nodes - d, length, d - nodes))
                for begin, end, shift in pieces:
                    for a in range(begin, end, 8):
                        n = min(8, end - a)
                        value = sums[pl.ds(base + a, n), :]
                        m0, n0 = 3 * a + i, 3 * (a + shift) + j
                        stride = 3 * pitch + 3
                        if n == 1:
                            out[pl.ds(m0 * pitch + n0, 1), :] = value
                            out[pl.ds(n0 * pitch + m0, 1), :] = value
                        else:
                            out[pl.ds(m0 * pitch + n0, n, stride=stride), :] = value
                            if d > 0:
                                out[pl.ds(n0 * pitch + m0, n, stride=stride), :] = value


def shards(nrow, ncol, grads, weights, counts, lame_first, shear, dest_owner, dest_slot):
    nq, nodes, _, count = grads.shape
    ndev = nrow * ncol
    ndof = 3 * nodes
    cap = max(2, 2 * count // ndev)
    cap = cap + (-cap) % 8
    width = ndev * cap
    half = nodes // 2
    packed = HEAD + 6 * nodes + 9 * nodes * (half - 1) + 9 * half
    total_rows = packed + (-packed) % LANES
    pitch = ndof + (-ndof) % 8
    gview = jnp.transpose(grads, (1, 2, 0, 3)).reshape(ndof * nq, count)
    row = lambda x: x.reshape(1, count)
    vmem = pl.BlockSpec(memory_space=pltpu.VMEM)
    steps = len(chunk_bounds(total_rows))
    sizes = (nodes, nq, nrow, ncol, cap, packed, total_rows, count * ndev)
    sums = pl.pallas_call(
        functools.partial(send_kernel, sizes),
        out_shape=jax.ShapeDtypeStruct((total_rows, LANES), F32),
        in_specs=[vmem] * 7,
        out_specs=vmem,
        scratch_shapes=[
            pltpu.VMEM((nq, 6 * nodes, LANES), F32),
            pltpu.VMEM((nq, 72, LANES), F32),
            pltpu.VMEM((total_rows, LANES), F32),
            pltpu.VMEM((width, total_rows), F32),
            pltpu.VMEM((width, total_rows), F32),
            pltpu.SemaphoreType.DMA((steps,)),
            pltpu.SemaphoreType.DMA((steps,)),
            pltpu.SemaphoreType.DMA((steps,)),
        ],
        compiler_params=pltpu.CompilerParams(
            collective_id=0, has_side_effects=True, vmem_limit_bytes=56 << 20),
        name="moments_exchange",
    )(gview, weights, row(counts), row(lame_first), row(shear), row(dest_owner), row(dest_slot))
    out = pl.pallas_call(
        functools.partial(mirror_kernel, nodes),
        out_shape=jax.ShapeDtypeStruct((ndof * pitch, LANES), F32),
        in_specs=[vmem],
        out_specs=vmem,
        compiler_params=pltpu.CompilerParams(vmem_limit_bytes=56 << 20),
        name="mirror",
    )(sums)
    return out.reshape(ndof, pitch, LANES)[:, :ndof, :]


def solution(mesh):
    both = ("row", "col")
    in_specs = (P(None, None, None, both), P(None, both), P(both), P(both), P(both),
                P(both, None), P(both))
    body = functools.partial(shards, mesh.shape["row"], mesh.shape["col"])
    return jax.shard_map(body, mesh=mesh, in_specs=in_specs, out_specs=P(None, None, both),
                         check_vma=False)
```

```python
import functools

import jax
import jax.numpy as jnp
from jax import lax
from jax.experimental import pallas as pl
from jax.experimental.pallas import tpu as pltpu
from jax.sharding import PartitionSpec as P

GP = 8
LANES = 128
HEAD = 8
BLOCKS = 4
TILES = (1, 2, 4, 6)
F32 = jnp.float32
BF16 = jnp.bfloat16
NT = (((1,), (1,)), ((), ()))


def split2(x):
    high = x.astype(BF16)
    return high, (x - high.astype(F32)).astype(BF16)


def row_base(d, nodes, i, j):
    half = nodes // 2
    if d == 0:
        i, j = min(i, j), max(i, j)
        return HEAD + (3 * i - i * (i + 1) // 2 + j) * nodes, nodes
    start = HEAD + 6 * nodes + (d - 1) * 9 * nodes
    if d < half:
        return start + (3 * i + j) * nodes, nodes
    return start + (3 * i + j) * half, half


def chunk_bounds(total_rows):
    cuts = [0]
    for tiles in TILES:
        if cuts[-1] + tiles * LANES < total_rows:
            cuts.append(cuts[-1] + tiles * LANES)
    return tuple(zip(cuts, cuts[1:] + [total_rows]))


def send_kernel(sizes, grads, weights, counts, lame, shear, owner, slot, sums,
                gbuf, wbuf, kbuf, send, recv, ssem, rsem, lsem):
    nodes, nq, nrow, ncol, cap, packed, total_rows, count_all = sizes
    ndev = nrow * ncol
    width = ndev * cap
    half = nodes // 2
    chunks = chunk_bounds(total_rows)
    me = lax.axis_index("row") * ncol + lax.axis_index("col")
    mine = pl.ds(pl.multiple_of(me * cap, 8), cap)
    most = pl.ds(0, (ndev - 1) * cap)

    def device(k):
        t = lax.rem(me + k, ndev)
        return t, (t // ncol, lax.rem(t, ncol))

    barrier = pltpu.get_barrier_semaphore()

    @pl.loop(1, ndev)
    def _(k):
        pl.semaphore_signal(barrier, inc=1, device_id=device(k)[1],
                            device_id_type=pl.DeviceIdType.MESH)

    span = 2 * nodes
    pad = 24

    def prepare(q, carry):
        weight = weights[pl.ds(q, 1), :]
        weight = jnp.where(q < counts[...] * GP, weight, 0.0)
        for i in range(3):
            values = grads[pl.ds(i * nq + q, nodes, stride=3 * nq), :]
            gbuf[q, pl.ds(i * span, nodes), :] = values
            gbuf[q, pl.ds(i * span + nodes, nodes), :] = values
            wbuf[q, pl.ds(i * pad, nodes), :] = values * weight
        return carry

    lax.fori_loop(0, nq, prepare, 0, unroll=4)

    who = owner[...].astype(F32)
    across = jnp.broadcast_to(who, (LANES, LANES))
    down = across.T
    first = lax.broadcasted_iota(jnp.int32, (LANES, LANES), 0)
    second = lax.broadcasted_iota(jnp.int32, (LANES, LANES), 1)
    same = jnp.where((across == down) & (first < second), 1.0, 0.0)
    rank = jnp.sum(same, axis=0, keepdims=True)
    position = (who * cap + rank).astype(jnp.int32)
    where = lax.broadcasted_iota(jnp.int32, (width, LANES), 0)
    onehot = jnp.where(where == position, 1.0, 0.0).astype(BF16)
    onehot2 = jnp.concatenate([onehot, onehot], axis=1)

    lam, mu = lame[...], shear[...]
    trace_row = jnp.zeros((1, LANES), F32)
    extra = lax.broadcasted_iota(jnp.int32, (HEAD, LANES), 0)
    kbuf[pl.ds(0, HEAD), :] = jnp.where(extra == 0, slot[...].astype(F32) + 1.0, 0.0)
    kbuf[pl.ds(packed, total_rows - packed), :] = jnp.zeros((total_rows - packed, LANES), F32)

    chunk = 0
    for d in range(half + 1):
        tiles = 3 if d < half else 2

        def step(q, acc, d=d, tiles=tiles):
            acc = list(acc)
            for t in range(tiles):
                left = [wbuf[q, pl.ds(i * pad + 8 * t, 8), :] for i in range(3)]
                right = [gbuf[q, pl.ds(j * span + d + 8 * t, 8), :] for j in range(3)]
                for i in range(3):
                    for j in range(3):
                        n = t * 9 + 3 * i + j
                        acc[n] = acc[n] + left[i] * right[j]
            return tuple(acc)

        zero = jnp.zeros((8, LANES), F32)
        acc = lax.fori_loop(0, nq, step, (zero,) * (9 * tiles), unroll=2)
        for t in range(tiles):
            m = acc[9 * t: 9 * t + 9]
            diag = m[0] + m[4] + m[8]
            _, length = row_base(d, nodes, 0, 0)
            rows = min(8, length - 8 * t)
            if d == 0:
                trace_row = trace_row + jnp.sum(diag[:rows], axis=0, keepdims=True)
            for i in range(3):
                for j in range(i if d == 0 else 0, 3):
                    value = lam * m[3 * i + j] + mu * m[3 * j + i]
                    if i == j:
                        value = value + mu * diag
                    base, _ = row_base(d, nodes, i, j)
                    kbuf[pl.ds(base + 8 * t, rows), :] = value[:rows]
        if d == 0:
            local = jnp.sum((lam + 4.0 * mu) * trace_row, axis=(0, 1), keepdims=True)
        done = total_rows if d == half else HEAD + 6 * nodes + 9 * nodes * d
        while chunk < len(chunks) and chunks[chunk][1] <= done:
            low_row, high_row = chunks[chunk]
            columns = pl.ds(low_row, high_row - low_row)
            high, low = split2(kbuf[columns, :])
            both = jnp.concatenate([high, low], axis=1)
            out = lax.dot_general(onehot2, both, NT, preferred_element_type=F32)
            if chunk == 0:
                column = lax.broadcasted_iota(jnp.int32, out.shape, 1)
                out = jnp.where(column == 1, local, out)
            send[:, columns] = out
            if chunk == 0:
                pl.semaphore_wait(barrier, ndev - 1)

            @pl.loop(1, ndev)
            def _(k, chunk=chunk, columns=columns):
                t, where_to = device(k)
                pltpu.make_async_remote_copy(
                    src_ref=send.at[pl.ds(pl.multiple_of(t * cap, 8), cap), columns],
                    dst_ref=recv.at[mine, columns],
                    send_sem=ssem.at[chunk], recv_sem=rsem.at[chunk],
                    device_id=where_to, device_id_type=pl.DeviceIdType.MESH).start()

            pltpu.make_async_copy(send.at[mine, columns], recv.at[mine, columns],
                                  lsem.at[chunk]).start()
            chunk += 1

    for c, (low_row, high_row) in enumerate(chunks):
        columns = pl.ds(low_row, high_row - low_row)
        pltpu.make_async_copy(send.at[mine, columns], recv.at[mine, columns], lsem.at[c]).wait()
        pltpu.make_async_copy(recv.at[most, columns], recv.at[most, columns], rsem.at[c]).wait()
        if c == 0:
            info = recv[:, 0:LANES]
            total = jnp.sum(info[:, 1:2], axis=0, keepdims=True) / cap
            inverse = (3 * nodes * count_all) / total
            lane = lax.broadcasted_iota(jnp.int32, (width, LANES), 1)
            placing = jnp.where(info[:, 0:1].astype(jnp.int32) == lane + 1, 1.0, 0.0)
            placing = placing.T.astype(BF16)
        high, low = split2(recv[:, columns])
        summed = jnp.dot(placing, high, preferred_element_type=F32)
        summed = summed + jnp.dot(placing, low, preferred_element_type=F32)
        sums[columns, :] = (summed * inverse).T
    for c, (low_row, high_row) in enumerate(chunks):
        columns = pl.ds(low_row, high_row - low_row)
        pltpu.make_async_copy(send.at[most, columns], send.at[most, columns], ssem.at[c]).wait()


def mirror_kernel(nodes, sums, out, obuf, osem):
    half = nodes // 2
    ndof = 3 * nodes
    pitch = ndof + (-ndof) % 8
    stride = 3 * pitch + 3
    block = nodes // BLOCKS
    copies = []

    def move(source, m0, n0, n):
        value = sums[pl.ds(source, n), :]
        if n == 1:
            obuf[pl.ds(m0 * pitch + n0, 1), :] = value
        else:
            obuf[pl.ds(m0 * pitch + n0, n, stride=stride), :] = value

    for first in range(0, nodes, block):
        for d in range(half + 1):
            for i in range(3):
                for j in range(3):
                    base, length = row_base(d, nodes, i, j)
                    for low, high, shift in ((0, nodes - d, d), (nodes - d, nodes, d - nodes)):
                        high = min(high, length)
                        begin, end = max(low, first), min(high, first + block)
                        for a in range(begin, end, 8):
                            n = min(8, end - a)
                            move(base + a, 3 * a + i, 3 * (a + shift) + j, n)
                        begin, end = max(low, first - shift), min(high, first - shift + block)
                        for a in range(begin, end, 8):
                            n = min(8, end - a)
                            if d > 0:
                                move(base + a, 3 * (a + shift) + j, 3 * a + i, n)
        rows = pl.ds(3 * first * pitch, 3 * block * pitch)
        copy = pltpu.make_async_copy(obuf.at[rows], out.at[rows], osem.at[first // block])
        copy.start()
        copies.append(copy)
    for copy in copies:
        copy.wait()


def shards(nrow, ncol, grads, weights, counts, lame_first, shear, dest_owner, dest_slot):
    nq, nodes, _, count = grads.shape
    ndev = nrow * ncol
    ndof = 3 * nodes
    cap = max(2, 2 * count // ndev)
    cap = cap + (-cap) % 8
    width = ndev * cap
    half = nodes // 2
    packed = HEAD + 6 * nodes + 9 * nodes * (half - 1) + 9 * half
    total_rows = packed + (-packed) % LANES
    pitch = ndof + (-ndof) % 8
    gview = jnp.transpose(grads, (1, 2, 0, 3)).reshape(ndof * nq, count)
    row = lambda x: x.reshape(1, count)
    vmem = pl.BlockSpec(memory_space=pltpu.VMEM)
    steps = len(chunk_bounds(total_rows))
    sizes = (nodes, nq, nrow, ncol, cap, packed, total_rows, count * ndev)
    sums = pl.pallas_call(
        functools.partial(send_kernel, sizes),
        out_shape=pltpu.VMEM((total_rows, LANES), F32),
        in_specs=[vmem] * 7,
        out_specs=vmem,
        scratch_shapes=[
            pltpu.VMEM((nq, 6 * nodes, LANES), F32),
            pltpu.VMEM((nq, 72, LANES), F32),
            pltpu.VMEM((total_rows, LANES), F32),
            pltpu.VMEM((width, total_rows), F32),
            pltpu.VMEM((width, total_rows), F32),
            pltpu.SemaphoreType.DMA((steps,)),
            pltpu.SemaphoreType.DMA((steps,)),
            pltpu.SemaphoreType.DMA((steps,)),
        ],
        compiler_params=pltpu.CompilerParams(
            collective_id=0, has_side_effects=True, vmem_limit_bytes=56 << 20),
        name="moments_exchange",
    )(gview, weights, row(counts), row(lame_first), row(shear), row(dest_owner), row(dest_slot))
    out = pl.pallas_call(
        functools.partial(mirror_kernel, nodes),
        out_shape=jax.ShapeDtypeStruct((ndof * pitch, LANES), F32),
        in_specs=[vmem],
        out_specs=pl.BlockSpec(memory_space=pl.ANY),
        scratch_shapes=[pltpu.VMEM((ndof * pitch, LANES), F32), pltpu.SemaphoreType.DMA((BLOCKS,))],
        compiler_params=pltpu.CompilerParams(vmem_limit_bytes=56 << 20),
        name="mirror",
    )(pltpu.with_memory_space_constraint(sums, pltpu.VMEM))
    return out.reshape(ndof, pitch, LANES)[:, :ndof, :]


def solution(mesh):
    both = ("row", "col")
    in_specs = (P(None, None, None, both), P(None, both), P(both), P(both), P(both),
                P(both, None), P(both))
    body = functools.partial(shards, mesh.shape["row"], mesh.shape["col"])
    return jax.shard_map(body, mesh=mesh, in_specs=in_specs, out_specs=P(None, None, both),
                         check_vma=False)
```
